64 devices in a mesh: dp: 8 (over x, y, core), tp: 8 (over z).
Axes of the slice: x: 2, y: 2, z: 8, core: 2. Of those that a mesh axis runs over, the one named last changes fastest.
The devices are a block of a 4x4x8 slice.
Arguments:
- x: bfloat16 [1024, 12288], P('dp'), parts along dimension 0
- w_gate: bfloat16 [12288, 33792], P(None, 'tp')
- w_up: bfloat16 [12288, 33792], P(None, 'tp')
- w_down: bfloat16 [33792, 12288], P('tp')
Outputs:
- output: bfloat16 [1024, 12288], P('dp'), parts along dimension 0
There are 8 independent parts. The reference program is written for one: setup_inputs(seed, part) draws one part's arguments, and reference() takes and returns one part's arrays. A program takes and returns all parts, laid end to end along the dimension named above; an argument that names none is the same for every part.
All inputs are finite; a program needn't handle non-finite values.
Results may differ from the reference program's by a relative error of at most 0.016.
Values are sent between devices in bfloat16 or wider.
A program may use at most 768 MiB of HBM per device.

```python
import jax
import jax.numpy as jnp

ROWS = 128
D = 12288
FF = 33792


def setup_inputs(seed: int = 0, part: int = 0) -> dict:
    kx, kg, ku, kd = jax.random.split(jax.random.key(seed), 4)
    drawn = {
        "x": jax.random.normal(jax.random.fold_in(kx, part), (ROWS, D), jnp.float32),
        "w_gate": jax.random.normal(kg, (D, FF), jnp.float32) * D**-0.5,
        "w_up": jax.random.normal(ku, (D, FF), jnp.float32) * D**-0.5,
        "w_down": jax.random.normal(kd, (FF, D), jnp.float32) * FF**-0.5,
    }
    return {k: v.astype(jnp.bfloat16) for k, v in drawn.items()}


def reference(x, w_gate, w_up, w_down):
    gate = jnp.dot(x, w_gate, preferred_element_type=jnp.float32)
    up = jnp.dot(x, w_up, preferred_element_type=jnp.float32)
    hidden = (jax.nn.silu(gate) * up).astype(jnp.bfloat16)
    return jnp.dot(hidden, w_down, preferred_element_type=jnp.float32).astype(jnp.bfloat16)
```

```python
import functools

import jax
import jax.numpy as jnp
from jax import lax
from jax.experimental import pallas as pl
from jax.experimental.pallas import tpu as pltpu
from jax.sharding import PartitionSpec as P

LANES = 128
SUBS = 3
SLABS = 16
SLAB_SLOTS = 3
DOWN_SLOTS = 4
MESH = pl.DeviceIdType.MESH
VMEM_BYTES = 67_043_328


def kernel(n, x_hbm, wg_hbm, wu_hbm, wd_hbm, y_hbm, xall, acc, hid, wbuf, dbuf, term, psend, precv,
           rsend, rrecv, ybuf, x_own_sem, x_send_sem, x_recv_sem, w_sem, d_sem, p_send_sem,
           p_recv_sem, r_send_sem, r_recv_sem, g_send_sem, g_recv_sem, y_sem):
    dp, tp = lax.axis_index("dp"), lax.axis_index("tp")
    half = lax.rem(dp, 2)
    partner = {"dp": dp + 1 - 2 * half}
    neighbour = ({"tp": lax.rem(tp + 1, n)}, {"tp": lax.rem(tp + n - 1, n)})

    rows, depth = x_hbm.shape
    slabs, _, slab = xall.shape
    width = hid.shape[1]
    local = wd_hbm.shape[0]
    first = pl.multiple_of(half * (local - width), LANES)
    overlap = 2 * width - local
    sub = ybuf.shape[1] // (2 * n * SUBS)
    chunk = sub * SUBS
    pairs = n * SUBS

    def weights(i, slot, act=lambda c: c.start()):
        k = pl.multiple_of(i * slab, LANES)
        for j, w in enumerate((wg_hbm, wu_hbm)):
            act(pltpu.make_async_copy(
                w.at[pl.ds(k, slab), pl.ds(first, width)],
                wbuf.at[slot, :, pl.ds(j * width, width)],
                w_sem.at[slot, j],
            ))

    def column(d, j, u):
        return pl.multiple_of((d * n + j) * chunk + u * sub, LANES)

    def ring_chunk(s, d):
        return lax.rem(tp + n - s, n) if d == 0 else lax.rem(tp + s, n)

    def down(s, u, act=lambda c: c.start()):
        slot = lax.rem(s * SUBS + u, DOWN_SLOTS)
        for d in range(2):
            act(pltpu.make_async_copy(
                wd_hbm.at[pl.ds(first, width), pl.ds(column(d, ring_chunk(s, d), u), sub)],
                dbuf.at[slot, :, pl.ds(d * sub, sub)],
                d_sem.at[slot, d],
            ))

    def own_copy(i):
        k = pl.multiple_of(i * slab, LANES)
        return pltpu.make_async_copy(
            x_hbm.at[:, pl.ds(k, slab)], xall.at[i, pl.ds(0, rows)], x_own_sem.at[i])

    def partner_copy(i):
        k = pl.multiple_of(i * slab, LANES)
        return pltpu.make_async_remote_copy(
            src_ref=x_hbm.at[:, pl.ds(k, slab)], dst_ref=xall.at[i, pl.ds(rows, rows)],
            send_sem=x_send_sem.at[i], recv_sem=x_recv_sem.at[i],
            device_id=partner, device_id_type=MESH)

    def term_copy(q):
        return pltpu.make_async_remote_copy(
            src_ref=psend.at[q], dst_ref=precv.at[q],
            send_sem=p_send_sem.at[q], recv_sem=p_recv_sem.at[q],
            device_id=partner, device_id_type=MESH)

    def ring_copy(s, u, d):
        i = s * SUBS + u
        return pltpu.make_async_remote_copy(
            src_ref=rsend.at[i, d], dst_ref=rrecv.at[i, d],
            send_sem=r_send_sem.at[i, d], recv_sem=r_recv_sem.at[i, d],
            device_id=neighbour[d], device_id_type=MESH)

    def gather_copy(a, u, d):
        j = ring_chunk(a - 1, d) if not (isinstance(a, int) and a == 0) else ring_chunk(n - 1, d)
        col = pl.ds(column(d, j, u), sub)
        i = a * SUBS + u
        return pltpu.make_async_remote_copy(
            src_ref=ybuf.at[:, col], dst_ref=ybuf.at[:, col],
            send_sem=g_send_sem.at[i, d], recv_sem=g_recv_sem.at[i, d],
            device_id=neighbour[d], device_id_type=MESH)

    def out_copy(a, u, d):
        j = ring_chunk(a, d) if a < n - 1 else ring_chunk(n - 1, d)
        col = pl.ds(column(d, j, u), sub)
        return pltpu.make_async_copy(ybuf.at[:, col], y_hbm.at[:, col], y_sem.at[a * SUBS + u, d])

    for i in range(slabs):
        own_copy(i).start()
        if i < SLAB_SLOTS:
            weights(i, i)
    barrier = pltpu.get_barrier_semaphore()
    for other in (partner,) + neighbour:
        pl.semaphore_signal(barrier, inc=1, device_id=other, device_id_type=MESH)
    pl.semaphore_wait(barrier, 3)
    for i in range(slabs):
        partner_copy(i).start()
    acc[...] = jnp.zeros_like(acc)

    def slab_ready(i, slot):
        own_copy(i).wait()
        partner_copy(i).wait_recv()
        weights(i, slot, lambda c: c.wait())

    @pl.loop(0, slabs - 1)
    def _(i):
        slot = lax.rem(i, SLAB_SLOTS)
        slab_ready(i, slot)
        acc[...] += jnp.dot(xall[i], wbuf[slot], preferred_element_type=jnp.float32)

        @pl.when(i + SLAB_SLOTS < slabs)
        def _():
            weights(i + SLAB_SLOTS, slot)

        @pl.when(i + SLAB_SLOTS == slabs - 1)
        def _():
            for q in range(DOWN_SLOTS):
                down(q // SUBS, q % SUBS)

    last = slabs - 1
    slot = last % SLAB_SLOTS
    slab_ready(last, slot)
    for c in range(0, width, 2 * LANES):
        w = min(2 * LANES, width - c)
        gate, up = (
            acc[:, c + o:c + o + w]
            + jnp.dot(xall[last], wbuf[slot, :, c + o:c + o + w], preferred_element_type=jnp.float32)
            for o in (0, width)
        )
        h = gate * jax.nn.sigmoid(gate) * up
        if c < overlap:
            unit = lax.broadcasted_iota(jnp.int32, h.shape, 1) + c
            h = jnp.where(unit < overlap * half, 0.0, h)
        hid[:, c:c + w] = h.astype(jnp.bfloat16)

    def matmul(s, u, more):
        q = s * SUBS + u
        slot = lax.rem(q, DOWN_SLOTS)
        down(s, u, lambda c: c.wait())
        t = jnp.dot(hid[...], dbuf[slot], preferred_element_type=jnp.float32)
        psend[q] = t[rows:].astype(jnp.bfloat16)
        term_copy(q).start()
        term[q] = t[:rows]
        if more:
            later = q + DOWN_SLOTS
            down(later // SUBS, lax.rem(later, SUBS))

    def pass_on(s, u):
        q = s * SUBS + u
        term_copy(q).wait_recv()
        start = isinstance(s, int) and s == 0
        end = isinstance(s, int) and s == n - 1
        for d in range(2):
            cut = slice(d * sub, (d + 1) * sub)
            v = term[q, :, cut] + precv[q, :, cut].astype(jnp.float32)
            if not start:
                ring_copy(s - 1, u, d).wait_recv()
                v = v + rrecv[(s - 1) * SUBS + u, d].astype(jnp.float32)
            v = v.astype(jnp.bfloat16)
            if end:
                ybuf[:, pl.ds(column(d, ring_chunk(n - 1, d), u), sub)] = v
                gather_copy(0, u, d).start()
                out_copy(n - 1, u, d).start()
            else:
                rsend[q, d] = v
                ring_copy(s, u, d).start()

    def step(s, behind):
        for u in range(SUBS):
            q = s * SUBS + u
            matmul(s, u, not isinstance(s, int) or q + DOWN_SLOTS < pairs)
            if u >= behind:
                pass_on(s, u - behind)
            elif not (isinstance(s, int) and s == 0):
                pass_on(s - 1, u - behind + SUBS)

    BEHIND = 2
    step(0, BEHIND)
    step(1, BEHIND)
    full = (pairs - DOWN_SLOTS) // SUBS

    @pl.loop(2, full)
    def _(s):
        step(s, BEHIND)

    for s in range(full, n):
        step(s, BEHIND)
    for u in range(SUBS - BEHIND, SUBS):
        pass_on(n - 1, u)

    for a in range(n - 1):
        for u in range(SUBS):
            for d in range(2):
                gather_copy(a, u, d).wait_recv()
                if a + 1 < n - 1:
                    gather_copy(a + 1, u, d).start()
                out_copy(a, u, d).start()

    for i in range(slabs):
        partner_copy(i).wait_send()
    for q in range(pairs):
        term_copy(q).wait_send()
    for a in range(n):
        for u in range(SUBS):
            for d in range(2):
                if a < n - 1:
                    ring_copy(a, u, d).wait_send()
                    gather_copy(a, u, d).wait_send()
                out_copy(a, u, d).wait()


def block(n, x, w_gate, w_up, w_down):
    rows, depth = x.shape
    local = w_down.shape[0]
    blocks = local // LANES
    width = (blocks + 1) // 2 * LANES
    slab = depth // SLABS
    sub = depth // (2 * n * SUBS)
    pairs = n * SUBS
    bf16, f32 = jnp.bfloat16, jnp.float32
    dma = pltpu.SemaphoreType.DMA
    return pl.pallas_call(
        functools.partial(kernel, n),
        out_shape=jax.ShapeDtypeStruct((rows, depth), bf16),
        in_specs=[pl.BlockSpec(memory_space=pl.ANY)] * 4,
        out_specs=pl.BlockSpec(memory_space=pl.ANY),
        scratch_shapes=[
            pltpu.VMEM((SLABS, 2 * rows, slab), bf16),
            pltpu.VMEM((2 * rows, 2 * width), f32),
            pltpu.VMEM((2 * rows, width), bf16),
            pltpu.VMEM((SLAB_SLOTS, slab, 2 * width), bf16),
            pltpu.VMEM((DOWN_SLOTS, width, 2 * sub), bf16),
            pltpu.VMEM((pairs, rows, 2 * sub), f32),
            pltpu.VMEM((pairs, rows, 2 * sub), bf16),
            pltpu.VMEM((pairs, rows, 2 * sub), bf16),
            pltpu.VMEM((pairs - SUBS, 2, rows, sub), bf16),
            pltpu.VMEM((pairs - SUBS, 2, rows, sub), bf16),
            pltpu.VMEM((rows, depth), bf16),
            dma((SLABS,)), dma((SLABS,)), dma((SLABS,)),
            dma((SLAB_SLOTS, 2)), dma((DOWN_SLOTS, 2)),
            dma((pairs,)), dma((pairs,)),
            dma((pairs - SUBS, 2)), dma((pairs - SUBS, 2)),
            dma((pairs - SUBS, 2)), dma((pairs - SUBS, 2)),
            dma((pairs, 2)),
        ],
        compiler_params=pltpu.CompilerParams(
            collective_id=0, has_side_effects=True, vmem_limit_bytes=VMEM_BYTES),
        name="mlp",
    )(x, w_gate, w_up, w_down)


def solution(mesh):
    n = mesh.shape["tp"]
    return jax.shard_map(
        functools.partial(block, n),
        mesh=mesh,
        in_specs=(P("dp", None), P(None, "tp"), P(None, "tp"), P("tp", None)),
        out_specs=P("dp", None),
        check_vma=False,
    )
```

```python
import functools

import jax
import jax.numpy as jnp
from jax import lax
from jax.experimental import pallas as pl
from jax.experimental.pallas import tpu as pltpu
from jax.sharding import PartitionSpec as P

LANES = 128
SUBS = 3
HALVES = 2
PARTS = 3
SLABS = 16
SLAB_SLOTS = 3
DOWN_SLOTS = 3
MESH = pl.DeviceIdType.MESH
VMEM_BYTES = 62_000_000


def kernel(n, x_hbm, wg_hbm, wu_hbm, wd_hbm, ybuf, xall, acc, hid, wbuf, dbuf, term, psend, precv,
           rsend, rrecv, x_own_sem, x_send_sem, x_recv_sem, w_sem, l_sem, d_sem, p_send_sem,
           p_recv_sem, r_send_sem, r_recv_sem, g_send_sem, g_recv_sem):
    dp, tp = lax.axis_index("dp"), lax.axis_index("tp")
    half = lax.rem(dp, 2)
    partner = {"dp": dp + 1 - 2 * half}
    neighbour = ({"tp": lax.rem(tp + 1, n)}, {"tp": lax.rem(tp + n - 1, n)})

    rows, depth = x_hbm.shape
    slabs, _, slab = xall.shape
    width = hid.shape[1]
    local = wd_hbm.shape[0]
    first = pl.multiple_of(half * (local - width), LANES)
    overlap = 2 * width - local
    sub = depth // (2 * n * SUBS)
    chunk = sub * SUBS
    pairs = n * SUBS
    pieces = SUBS * HALVES
    piece = sub // HALVES
    last = slabs - 1
    cuts = [c * 2 * LANES for c in range(-(-width // (2 * LANES)))]
    parts = [cuts[p * len(cuts) // PARTS] for p in range(PARTS)] + [width]

    def weights(i, slot, act=lambda c: c.start()):
        k = pl.multiple_of(i * slab, LANES)
        for j, w in enumerate((wg_hbm, wu_hbm)):
            act(pltpu.make_async_copy(
                w.at[pl.ds(k, slab), pl.ds(first, width)],
                wbuf.at[slot, :, pl.ds(j * width, width)],
                w_sem.at[slot, j],
            ))

    def last_weights(p, act=lambda c: c.start()):
        a, b = parts[p], parts[p + 1]
        for j, w in enumerate((wg_hbm, wu_hbm)):
            act(pltpu.make_async_copy(
                w.at[pl.ds(last * slab, slab), pl.ds(pl.multiple_of(first + a, LANES), b - a)],
                wbuf.at[last % SLAB_SLOTS, :, pl.ds(j * width + a, b - a)],
                l_sem.at[p, j],
            ))

    def column(d, j, u):
        return pl.multiple_of((d * n + j) * chunk + u * sub, LANES)

    def ring_chunk(s, d):
        return lax.rem(tp + n - s, n) if d == 0 else lax.rem(tp + s, n)

    def down(s, u, act=lambda c: c.start()):
        slot = lax.rem(s * SUBS + u, DOWN_SLOTS)
        for d in range(2):
            act(pltpu.make_async_copy(
                wd_hbm.at[pl.ds(first, width), pl.ds(column(d, ring_chunk(s, d), u), sub)],
                dbuf.at[slot, :, pl.ds(d * sub, sub)],
                d_sem.at[slot, d],
            ))

    def own_copy(i):
        k = pl.multiple_of(i * slab, LANES)
        return pltpu.make_async_copy(
            x_hbm.at[:, pl.ds(k, slab)], xall.at[i, pl.ds(0, rows)], x_own_sem.at[i])

    def partner_copy(i):
        k = pl.multiple_of(i * slab, LANES)
        return pltpu.make_async_remote_copy(
            src_ref=x_hbm.at[:, pl.ds(k, slab)], dst_ref=xall.at[i, pl.ds(rows, rows)],
            send_sem=x_send_sem.at[i], recv_sem=x_recv_sem.at[i],
            device_id=partner, device_id_type=MESH)

    def term_copy(q):
        return pltpu.make_async_remote_copy(
            src_ref=psend.at[q], dst_ref=precv.at[q],
            send_sem=p_send_sem.at[q], recv_sem=p_recv_sem.at[q],
            device_id=partner, device_id_type=MESH)

    def ring_copy(s, p, d):
        i = s * pieces + p
        return pltpu.make_async_remote_copy(
            src_ref=rsend.at[i, d], dst_ref=rrecv.at[i, d],
            send_sem=r_send_sem.at[i, d], recv_sem=r_recv_sem.at[i, d],
            device_id=neighbour[d], device_id_type=MESH)

    def place(j, p, d):
        return (d * n + j) * pieces + p

    def gather_copy(a, p, d):
        at = place(ring_chunk(n - 1 if a == 0 else a - 1, d), p, d)
        i = a * pieces + p
        return pltpu.make_async_remote_copy(
            src_ref=ybuf.at[at], dst_ref=ybuf.at[at],
            send_sem=g_send_sem.at[i, d], recv_sem=g_recv_sem.at[i, d],
            device_id=neighbour[d], device_id_type=MESH)

    for i in range(slabs):
        own_copy(i).start()
        if i < SLAB_SLOTS:
            weights(i, i)
    barrier = pltpu.get_barrier_semaphore()
    for other in (partner,) + neighbour:
        pl.semaphore_signal(barrier, inc=1, device_id=other, device_id_type=MESH)
    pl.semaphore_wait(barrier, 3)
    for i in range(slabs):
        partner_copy(i).start()
    acc[...] = jnp.zeros_like(acc)

    def rows_ready(i):
        own_copy(i).wait()
        partner_copy(i).wait_recv()

    @pl.loop(0, slabs - 1)
    def _(i):
        slot = lax.rem(i, SLAB_SLOTS)
        rows_ready(i)
        weights(i, slot, lambda c: c.wait())
        acc[...] += jnp.dot(xall[i], wbuf[slot], preferred_element_type=jnp.float32)

        @pl.when(i + SLAB_SLOTS < last)
        def _():
            weights(i + SLAB_SLOTS, slot)

        @pl.when(i + SLAB_SLOTS == last)
        def _():
            for p in range(PARTS):
                last_weights(p)
            for q in range(DOWN_SLOTS):
                down(q // SUBS, q % SUBS)

    slot = last % SLAB_SLOTS
    rows_ready(last)
    for c in cuts:
        if c in parts:
            last_weights(parts.index(c), lambda c: c.wait())
        w = min(2 * LANES, width - c)
        gate, up = (
            acc[:, c + o:c + o + w]
            + jnp.dot(xall[last], wbuf[slot, :, c + o:c + o + w], preferred_element_type=jnp.float32)
            for o in (0, width)
        )
        h = gate * jax.nn.sigmoid(gate) * up
        if c < overlap:
            unit = lax.broadcasted_iota(jnp.int32, h.shape, 1) + c
            h = jnp.where(unit < overlap * half, 0.0, h)
        hid[:, c:c + w] = h.astype(jnp.bfloat16)

    def matmul(s, u, more):
        q = s * SUBS + u
        slot = lax.rem(q, DOWN_SLOTS)
        down(s, u, lambda c: c.wait())
        t = jnp.dot(hid[...], dbuf[slot], preferred_element_type=jnp.float32)
        psend[q] = t[rows:].astype(jnp.bfloat16)
        term_copy(q).start()
        term[q] = t[:rows]
        if more:
            later = q + DOWN_SLOTS
            down(later // SUBS, lax.rem(later, SUBS))

    def pass_on(s, u):
        q = s * SUBS + u
        term_copy(q).wait_recv()
        start = isinstance(s, int) and s == 0
        end = isinstance(s, int) and s == n - 1
        for h in range(HALVES):
            for d in range(2):
                p = u * HALVES + h
                cut = slice(d * sub + h * piece, d * sub + (h + 1) * piece)
                v = term[q, :, cut] + precv[q, :, cut].astype(jnp.float32)
                if not start:
                    ring_copy(s - 1, p, d).wait_recv()
                    v = v + rrecv[(s - 1) * pieces + p, d].astype(jnp.float32)
                v = v.astype(jnp.bfloat16)
                if end:
                    ybuf[place(ring_chunk(n - 1, d), p, d)] = v
                    gather_copy(0, p, d).start()
                else:
                    rsend[s * pieces + p, d] = v
                    ring_copy(s, p, d).start()

    def step(s, behind):
        for u in range(SUBS):
            q = s * SUBS + u
            matmul(s, u, not isinstance(s, int) or q + DOWN_SLOTS < pairs)
            if u >= behind:
                pass_on(s, u - behind)
            elif not (isinstance(s, int) and s == 0):
                pass_on(s - 1, u - behind + SUBS)

    BEHIND = 2
    step(0, BEHIND)
    step(1, BEHIND)
    full = (pairs - DOWN_SLOTS) // SUBS

    @pl.loop(2, full)
    def _(s):
        step(s, BEHIND)

    for s in range(full, n):
        step(s, BEHIND)
    for u in range(SUBS - BEHIND, SUBS):
        pass_on(n - 1, u)

    for a in range(n - 1):
        for p in range(pieces):
            for d in range(2):
                gather_copy(a, p, d).wait_recv()
                if a + 1 < n - 1:
                    gather_copy(a + 1, p, d).start()

    for i in range(slabs):
        partner_copy(i).wait_send()
    for q in range(pairs):
        term_copy(q).wait_send()
    for a in range(n - 1):
        for p in range(pieces):
            for d in range(2):
                ring_copy(a, p, d).wait_send()
                gather_copy(a, p, d).wait_send()


def lay_out(blocks, y_hbm, sem):
    count, _, piece = blocks.shape
    copies = [
        pltpu.make_async_copy(blocks.at[i], y_hbm.at[:, pl.ds(i * piece, piece)], sem.at[i])
        for i in range(count)
    ]
    for copy in copies:
        copy.start()
    for copy in copies:
        copy.wait()


def block(n, x, w_gate, w_up, w_down):
    rows, depth = x.shape
    local = w_down.shape[0]
    blocks = local // LANES
    width = (blocks + 1) // 2 * LANES
    slab = depth // SLABS
    sub = depth // (2 * n * SUBS)
    pairs = n * SUBS
    pieces = SUBS * HALVES
    piece = sub // HALVES
    bf16, f32 = jnp.bfloat16, jnp.float32
    dma = pltpu.SemaphoreType.DMA
    ring = (n - 1) * pieces
    blocks = pl.pallas_call(
        functools.partial(kernel, n),
        out_shape=pltpu.VMEM((2 * n * pieces, rows, piece), bf16),
        in_specs=[pl.BlockSpec(memory_space=pl.ANY)] * 4,
        out_specs=pl.BlockSpec(memory_space=pltpu.VMEM),
        scratch_shapes=[
            pltpu.VMEM((SLABS, 2 * rows, slab), bf16),
            pltpu.VMEM((2 * rows, 2 * width), f32),
            pltpu.VMEM((2 * rows, width), bf16),
            pltpu.VMEM((SLAB_SLOTS, slab, 2 * width), bf16),
            pltpu.VMEM((DOWN_SLOTS, width, 2 * sub), bf16),
            pltpu.VMEM((pairs, rows, 2 * sub), f32),
            pltpu.VMEM((pairs, rows, 2 * sub), bf16),
            pltpu.VMEM((pairs, rows, 2 * sub), bf16),
            pltpu.VMEM((ring, 2, rows, piece), bf16),
            pltpu.VMEM((ring, 2, rows, piece), bf16),
            dma((SLABS,)), dma((SLABS,)), dma((SLABS,)),
            dma((SLAB_SLOTS, 2)), dma((PARTS, 2)), dma((DOWN_SLOTS, 2)),
            dma((pairs,)), dma((pairs,)),
            dma((ring, 2)), dma((ring, 2)), dma((ring, 2)), dma((ring, 2)),
        ],
        compiler_params=pltpu.CompilerParams(
            collective_id=0, has_side_effects=True, vmem_limit_bytes=VMEM_BYTES),
        name="mlp",
    )(x, w_gate, w_up, w_down)
    return pl.pallas_call(
        lay_out,
        out_shape=jax.ShapeDtypeStruct((rows, depth), bf16),
        in_specs=[pl.BlockSpec(memory_space=pltpu.VMEM)],
        out_specs=pl.BlockSpec(memory_space=pl.ANY),
        scratch_shapes=[dma((2 * n * pieces,))],
        compiler_params=pltpu.CompilerParams(vmem_limit_bytes=1 << 22),
        name="lay_out",
    )(blocks)


def solution(mesh):
    n = mesh.shape["tp"]
    return jax.shard_map(
        functools.partial(block, n),
        mesh=mesh,
        in_specs=(P("dp", None), P(None, "tp"), P(None, "tp"), P("tp", None)),
        out_specs=P("dp", None),
        check_vma=False,
    )
```
